512 devices in a mesh: region: 128 (over z_hi, y, x), member: 4 (over z_lo, core).
Axes of the slice: x: 4, y: 8, z: 8 (z_hi: 4, z_lo: 2; z = z_hi * 2 + z_lo), core: 2. Of those that a mesh axis runs over, the one named last changes fastest.
Arguments:
- ensemble: float32 [4, 1024, 8192], P('member', 'region'), may hold values from -9 to 15, as said below
- band_index: int32 [4, 1024, 8192], P('member', 'region'), may hold values from 0 to 63
- region_cells: int32 [128], P('region'), may hold values from 8192 to 65536, as said below
- target_means: float32 [128, 64], P('region'), may hold values from -8 to 8
Outputs:
- corrected: float32 [4, 1024, 8192], P('member', 'region')
The draws below stay inside these ranges and needn't reach their ends.
Inputs may be any that keep to these rules, and one draw needn't show every extreme that they name: `ensemble`: finite values. `region_cells`: at least one eighth of a tile; one region in every draw holds its whole tile.
All inputs are finite; a program needn't handle non-finite values.
Results may differ from the reference program's by a relative error of at most 0.000057.
Values sent between devices are 32-bit elements; how exact they have to be, the bound alone decides.
No kernel may reach another device: no remote copies, remote signals or barrier semaphores. Data moves between devices by JAX's collectives and lax.ppermute only.
A program may use at most 64 MiB of HBM per device.

```python
import jax
import jax.numpy as jnp

LAT_DEV = 8
NLON = 8192
BANDS = 64
MEMBERS = 4
REGIONS = 128
NLAT = 1024


def common_bands(key):
    band_key = jax.random.fold_in(key, 41)
    return jax.random.randint(band_key, (MEMBERS, NLAT, NLON), 0, BANDS, dtype=jnp.int32)


def band_levels(key):
    level_key = jax.random.fold_in(key, 43)
    return jax.random.uniform(level_key, (BANDS,), jnp.float32, -4.0, 4.0)


def draw_band_index(key, part):
    return common_bands(key)


def draw_ensemble(key, part):
    base = jax.random.fold_in(key, 17)
    first, second = jax.random.split(base, 2)
    member_pos = jnp.arange(MEMBERS, dtype=jnp.float32) / max(MEMBERS - 1, 1)
    latitude_term = jax.random.uniform(first, (NLAT,), jnp.float32, -3.0, 3.0)
    bands = common_bands(key)
    levels = band_levels(key)
    band_term = jnp.take(levels, bands)
    member_mean = 1.0 + 2.0 * member_pos
    noise = jnp.clip(jax.random.normal(second, (MEMBERS, NLAT, NLON), jnp.float32), -3.0, 3.0)
    return member_mean[:, None, None] + latitude_term[None, :, None] + noise + band_term


def draw_region_cells(key, part):
    base = jax.random.fold_in(key, 29)
    first, second = jax.random.split(base, 2)
    whole = LAT_DEV * NLON
    counted = jax.random.randint(first, (REGIONS,), whole // 8, whole + 1, dtype=jnp.int32)
    chosen = jax.random.randint(second, (), 0, REGIONS, dtype=jnp.int32)
    return jnp.where(jnp.arange(REGIONS, dtype=jnp.int32) == chosen, whole, counted).astype(jnp.int32)


def block_levels(rng, extent, pieces, least, largest):
    factor_of, own = 1.0, jax.random.fold_in(rng, 6)
    for axis_at, parts in pieces:
        steps = jnp.exp(jax.random.uniform(jax.random.fold_in(own, axis_at), (parts,), jnp.float32, least / len(pieces), largest / len(pieces)))
        factor_of = factor_of * jnp.repeat(steps, extent[axis_at] // parts).reshape([-1 if axis == axis_at else 1 for axis in range(len(extent))])
    return factor_of


def gaussian(stream_key, dims, spread, most, cuts=(), held_as=jnp.bfloat16):
    result = jax.random.normal(stream_key, dims, jnp.float32) * spread
    if len(cuts) > 0:
        result = block_levels(stream_key, dims, cuts, -0.22, 0.18) * result
    return jnp.clip(result, min=-most, max=most).astype(held_as)


def setup_inputs(seed: int = 0) -> dict:
    key_list = jax.random.split(jax.random.key(seed), 5)
    return {
        "ensemble": draw_ensemble(jax.random.fold_in(key_list[4], 71), 0),
        "band_index": draw_band_index(jax.random.fold_in(key_list[4], 71), 0),
        "region_cells": draw_region_cells(jax.random.fold_in(key_list[4], 71), 0),
        "target_means": gaussian(key_list[3], (REGIONS, BANDS), 2.0, 8.0, ((0, 128),), jnp.float32),
    }


def smooth_pass(extended):
    vertical = extended[:, :-2] + 2.0 * extended[:, 1:-1] + extended[:, 2:]
    across = jnp.roll(vertical, 1, axis=2) + 2.0 * vertical + jnp.roll(vertical, -1, axis=2)
    return across / 16.0


def reference(ensemble, band_index, region_cells, target_means):
    smoothed = ensemble
    for repeat in range(2):
        smoothed = smooth_pass(jnp.pad(smoothed, ((0, 0), (1, 1), (0, 0)), mode="edge"))
    latitude = jnp.arange(NLAT, dtype=jnp.int32)
    region_of = latitude // LAT_DEV
    position = (latitude % LAT_DEV)[:, None] * NLON + jnp.arange(NLON, dtype=jnp.int32)[None, :]
    valid = (position < region_cells[region_of][:, None]).astype(jnp.float32)
    segment = (region_of[None, :, None] * BANDS + band_index).astype(jnp.int32)
    weighted = smoothed * valid[None]
    live = jnp.broadcast_to(valid[None], smoothed.shape)
    sums = jax.ops.segment_sum(weighted.ravel(), segment.ravel(), REGIONS * BANDS).reshape(REGIONS, BANDS)
    cells = jax.ops.segment_sum(live.ravel(), segment.ravel(), REGIONS * BANDS).reshape(REGIONS, BANDS)
    sums_pad = jnp.pad(sums, ((1, 1), (0, 0)))
    cells_pad = jnp.pad(cells, ((1, 1), (0, 0)))
    pooled_sums = sums_pad[:-2] + sums_pad[1:-1] + sums_pad[2:]
    pooled_cells = cells_pad[:-2] + cells_pad[1:-1] + cells_pad[2:]
    offset = target_means - pooled_sums / (pooled_cells + 1.0)
    applied = offset[region_of[None, :, None], band_index]
    return smoothed + valid[None] * applied
```

```python
import functools

import jax
import jax.numpy as jnp
from jax import lax
from jax.experimental import pallas as pl
from jax.experimental.pallas import tpu as pltpu
from jax.sharding import PartitionSpec as P

LANES = 128
LOW = 32


def smooth_rows(center, before, after, at_north, at_south):
    rows = center.shape[0]
    row = lax.broadcasted_iota(jnp.int32, center.shape, 0)
    first, last = row == 0, row == rows - 1
    north, south = center[0:1], center[rows - 1 : rows]
    above = jnp.where(at_north, north, before[1:2])
    below = jnp.where(at_south, south, after[0:1])

    def vertical(field, prior, later):
        up = jnp.where(first, prior, pltpu.roll(field, 1, 0))
        down = jnp.where(last, later, pltpu.roll(field, rows - 1, 0))
        return (up + 2.0 * field + down) * 0.25

    once = vertical(center, above, below)
    outer_above = (before[0:1] + 2.0 * above + north) * 0.25
    outer_below = (south + 2.0 * below + after[1:2]) * 0.25
    outer_above = jnp.where(at_north, once[0:1], outer_above)
    outer_below = jnp.where(at_south, once[rows - 1 : rows], outer_below)
    twice = vertical(once, outer_above, outer_below)
    width = center.shape[1]
    for _ in range(2):
        west, east = pltpu.roll(twice, 1, 1), pltpu.roll(twice, width - 1, 1)
        twice = (west + 2.0 * twice + east) * 0.25
    return twice


def live_mask(cells, shape):
    row = lax.broadcasted_iota(jnp.int32, shape, 0)
    column = lax.broadcasted_iota(jnp.int32, shape, 1)
    return row * shape[1] + column < cells


def stats_kernel(bands_total, cells_ref, place_ref, center_ref, inner_ref, outer_ref, band_ref, smoothed_ref, stats_ref):
    at_north, at_south, even = place_ref[0] != 0, place_ref[1] != 0, place_ref[2] != 0
    inner, outer = inner_ref[...], outer_ref[...]
    before, after = jnp.where(even, outer, inner), jnp.where(even, inner, outer)
    smoothed = smooth_rows(center_ref[...], before, after, at_north, at_south)
    smoothed_ref[...] = smoothed
    rows = smoothed.shape[0]
    live = live_mask(cells_ref[0], smoothed.shape)
    weighted = jnp.where(live, smoothed, 0.0)
    count = jnp.where(live, 1.0, 0.0)
    high = weighted.astype(jnp.bfloat16).astype(jnp.float32)
    rest = weighted - high
    middle = rest.astype(jnp.bfloat16).astype(jnp.float32)
    low = rest - middle
    terms = [high, middle, low, count]
    band = band_ref[...]
    upper, lower = band // LOW, band % LOW
    blocks = bands_total // LOW
    left = jnp.concatenate(
        [jnp.where(upper == a, t, 0.0) for a in range(blocks) for t in terms], axis=0
    ).astype(jnp.bfloat16)
    right = jnp.concatenate(
        [jnp.where(lower == b, 1.0, 0.0) for b in range(LOW)], axis=0
    ).astype(jnp.bfloat16)
    product = lax.dot_general(left, right, (((1,), (1,)), ((), ())), preferred_element_type=jnp.float32)
    row = lax.broadcasted_iota(jnp.int32, product.shape, 0)
    column = lax.broadcasted_iota(jnp.int32, product.shape, 1)
    kept = jnp.where(row % rows == column % rows, product, 0.0)
    spans = [jnp.sum(kept[k * rows : (k + 1) * rows], axis=0, keepdims=True) for k in range(blocks * 4)]
    total = None
    for a in range(blocks):
        for what in range(2):
            if what == 0:
                line = spans[4 * a] + (spans[4 * a + 1] + spans[4 * a + 2])
            else:
                line = spans[4 * a + 3]
            source = lax.broadcasted_iota(jnp.int32, (line.shape[1], 2 * bands_total), 0)
            target = lax.broadcasted_iota(jnp.int32, (line.shape[1], 2 * bands_total), 1)
            place = jnp.where(source // rows + (a * LOW + what * bands_total) == target, 1.0, 0.0)
            part = lax.dot_general(
                jnp.broadcast_to(line, (8, line.shape[1])), place, (((1,), (0,)), ((), ())),
                precision=lax.Precision.HIGHEST, preferred_element_type=jnp.float32,
            )
            total = part if total is None else total + part
    stats_ref[...] = total[0:1]


def apply_kernel(bands_total, cells_ref, total_ref, before_ref, after_ref, target_ref, band_ref, smoothed_ref, out_ref):
    pooled = before_ref[...] + total_ref[...] + after_ref[...]
    pooled = jnp.broadcast_to(pooled, (8, LANES))
    counts = pltpu.roll(pooled, LANES - bands_total, 1)
    target = jnp.concatenate([target_ref[...]] * (LANES // bands_total), axis=1)
    table = target - pooled / (counts + 1.0)
    cells = cells_ref[0]
    rows, width = band_ref.shape
    row = lax.broadcasted_iota(jnp.int32, (rows, LANES), 0)
    column = lax.broadcasted_iota(jnp.int32, (rows, LANES), 1)
    position = row * width + column
    for k in range(width // LANES):
        here = slice(k * LANES, (k + 1) * LANES)
        applied = jnp.take_along_axis(table, band_ref[:, here], axis=1, mode="promise_in_bounds")
        live = position + k * LANES < cells
        out_ref[:, here] = smoothed_ref[:, here] + jnp.where(live, applied, 0.0)


def shards(ensemble, band_index, region_cells, target_means):
    region_count = lax.axis_size("region")
    rank = lax.axis_index("region")
    _, rows, width = ensemble.shape
    bands_total = target_means.shape[1]
    inner_pairs = [(i, i ^ 1) for i in range(region_count)]
    outer_pairs = [(i, ((i + 1) ^ 1) - 1) for i in range(1, region_count - 1)]
    field, band = ensemble[0], band_index[0]
    even = rank % 2 == 0
    first, last = field[:2], field[rows - 2 :]
    outer = lax.ppermute(jnp.where(even, first, last), "region", outer_pairs)
    inner = lax.ppermute(jnp.where(even, last, first), "region", inner_pairs)
    places = jnp.stack([rank == 0, rank == region_count - 1, even]).astype(jnp.int32)
    smem, vmem = pl.BlockSpec(memory_space=pltpu.SMEM), pl.BlockSpec(memory_space=pltpu.VMEM)
    params = pltpu.CompilerParams(vmem_limit_bytes=16 * 2**20)
    smoothed, stats = pl.pallas_call(
        functools.partial(stats_kernel, bands_total),
        out_shape=(
            jax.ShapeDtypeStruct((rows, width), jnp.float32),
            jax.ShapeDtypeStruct((1, 2 * bands_total), jnp.float32),
        ),
        in_specs=[smem, smem, vmem, vmem, vmem, vmem],
        out_specs=(vmem, vmem),
        compiler_params=params,
        name="smooth_stats",
    )(region_cells, places, field, inner, outer, band)
    total = lax.all_gather(stats, "member").sum(axis=0)
    prior = lax.ppermute(total, "region", outer_pairs)
    later = lax.ppermute(total, "region", inner_pairs)
    out = pl.pallas_call(
        functools.partial(apply_kernel, bands_total),
        out_shape=jax.ShapeDtypeStruct((rows, width), jnp.float32),
        in_specs=[smem] + [vmem] * 6,
        out_specs=vmem,
        compiler_params=params,
        name="apply",
    )(region_cells, total, prior, later, target_means, band, smoothed)
    return out[None]


def solution(mesh):
    placed = (
        P("member", "region", None),
        P("member", "region", None),
        P("region"),
        P("region", None),
    )
    return jax.shard_map(
        shards, mesh=mesh, in_specs=placed, out_specs=P("member", "region", None), check_vma=False
    )
```

```python
import functools

import jax
import jax.numpy as jnp
from jax import lax
from jax.experimental import pallas as pl
from jax.experimental.pallas import tpu as pltpu
from jax.sharding import PartitionSpec as P

LANES = 128
SUBLANES = 8
LOW = 32


def iota(shape, axis):
    return lax.broadcasted_iota(jnp.int32, shape, axis)


def west_east(field):
    half, width = SUBLANES // 2, field.shape[1]
    lane = iota(field.shape, 1)
    west, east = pltpu.roll(field, 1, 1), pltpu.roll(field, width - 1, 1)
    west = jnp.where(lane == 0, pltpu.roll(west, half, 0), west)
    east = jnp.where(lane == width - 1, pltpu.roll(east, half, 0), east)
    return west, east


def bf16_terms(values):
    high = values.astype(jnp.bfloat16).astype(jnp.float32)
    rest = values - high
    middle = rest.astype(jnp.bfloat16).astype(jnp.float32)
    return [high, middle, rest - middle]


def band_lines(bands_total, code, groups):
    blocks = bands_total // LOW
    upper, lower = code // LOW, code % LOW
    terms = [t for group in groups for t in group]
    left = jnp.concatenate(
        [jnp.where(upper == a, t, 0.0) for a in range(blocks) for t in terms], axis=0
    ).astype(jnp.bfloat16)
    right = jnp.concatenate(
        [jnp.where(lower == b, 1.0, 0.0) for b in range(LOW)], axis=0
    ).astype(jnp.bfloat16)
    product = lax.dot_general(left, right, (((1,), (1,)), ((), ())), preferred_element_type=jnp.float32)
    kept = jnp.where(iota(product.shape, 0) % SUBLANES == iota(product.shape, 1) % SUBLANES, product, 0.0)
    lines, at = [], 0
    for a in range(blocks):
        for group in groups:
            block = kept[at * SUBLANES : (at + 1) * SUBLANES]
            for k in range(1, len(group)):
                block = block + kept[(at + k) * SUBLANES : (at + k + 1) * SUBLANES]
            at += len(group)
            lines.append(jnp.sum(block, axis=0, keepdims=True))
    sublane = iota((SUBLANES, product.shape[1]), 0)
    stacked = jnp.zeros((SUBLANES, product.shape[1]), jnp.float32)
    for k, line in enumerate(lines):
        stacked = jnp.where(sublane == k, line, stacked)
    width = stacked.shape[1]
    for shift in (1, 2, 4):
        stacked = stacked + pltpu.roll(stacked, width - shift, 1)
    lane = iota((SUBLANES, LANES), 1)
    per = LANES // SUBLANES
    pick = (lane % per) * SUBLANES
    placed = None
    for k in range(width // LANES):
        part = jnp.take_along_axis(stacked[:, k * LANES : (k + 1) * LANES], pick, axis=1, mode="promise_in_bounds")
        placed = part if placed is None else jnp.where((lane % LOW) // per == k, part, placed)
    total = None
    for a in range(blocks):
        for g in range(len(groups)):
            here = (iota((SUBLANES, LANES), 0) == a * len(groups) + g) & (lane // LOW == g * blocks + a)
            part = jnp.where(here, placed, 0.0)
            total = part if total is None else total + part
    return jnp.sum(total, axis=0, keepdims=True)


def packed_edges(field):
    half = field.shape[1] // 2
    west, east = pltpu.roll(field[:, :half], 2, 0), pltpu.roll(field[:, half:], 6, 0)
    return jnp.where(iota(west.shape, 0) < SUBLANES // 2, west, east)


def prepare_kernel(bands_total, cells_ref, place_ref, center_ref, band_ref, base_ref, code_ref, stats_ref):
    at_north, at_south = place_ref[0] != 0, place_ref[1] != 0
    center, band = center_ref[...], band_ref[...]
    rows, width = center.shape
    row = iota(center.shape, 0)
    first, last = row == 0, row == rows - 1
    north, south = center[0:1], center[rows - 1 : rows]

    def vertical(field, prior, later):
        up = jnp.where(first, prior, pltpu.roll(field, 1, 0))
        down = jnp.where(last, later, pltpu.roll(field, rows - 1, 0))
        return (up + 2.0 * field + down) * 0.25

    once = vertical(center, jnp.where(at_north, north, 0.0), jnp.where(at_south, south, 0.0))
    prior = jnp.where(at_north, once[0:1], north * 0.25)
    later = jnp.where(at_south, once[rows - 1 : rows], south * 0.25)
    base = vertical(once, prior, later)
    for _ in range(2):
        base = (pltpu.roll(base, 1, 1) + 2.0 * base + pltpu.roll(base, width - 1, 1)) * 0.25
    base_ref[...] = base
    live = row * width + iota(center.shape, 1) < cells_ref[0]
    code = jnp.where(live, band, bands_total)
    code_ref[...] = packed_edges(code)
    ones = jnp.full(base.shape, 1.0, jnp.float32)
    stats_ref[...] = band_lines(bands_total, code, [bf16_terms(base), [ones]])


def edges_kernel(bands_total, place_ref, inner_ref, outer_ref, base_ref, code_ref, prepared_ref, smoothed_ref, stats_ref):
    even = place_ref[2] != 0
    rows, width = base_ref.shape
    half = width // 2
    shape = (SUBLANES, half)
    slot = iota((SUBLANES, LANES), 0) % (SUBLANES // 2)
    low = iota(shape, 0) < SUBLANES // 2

    def weights(a, b, c, d):
        table = jnp.where(slot == 0, a, jnp.where(slot == 1, b, jnp.where(slot == 2, c, d)))
        return jnp.concatenate([table * (1.0 / 16.0)] * (half // LANES), axis=1)

    after = [weights(1.0, 4.0, 0.0, 0.0), weights(0.0, 1.0, 0.0, 0.0)]
    before = [weights(0.0, 0.0, 1.0, 0.0), weights(0.0, 0.0, 4.0, 1.0)]
    added = None
    for j in range(2):
        for ref, one, other in ((inner_ref, after, before), (outer_ref, before, after)):
            line = jnp.where(low, ref[j : j + 1, :half], ref[j : j + 1, half:])
            term = line * jnp.where(even, one[j], other[j])
            added = term if added is None else added + term
    for _ in range(2):
        west, east = west_east(added)
        added = (west + 2.0 * added + east) * 0.25
    stats = band_lines(bands_total, code_ref[...], [bf16_terms(added)])
    spread = iota(stats.shape, 1) < bands_total
    stats_ref[...] = prepared_ref[...] + jnp.where(spread, stats, 0.0)
    row = iota(shape, 0)
    edge = (row < 2) | (row >= rows - 2)
    smoothed_ref[:, :half] = base_ref[:, :half] + jnp.where(edge, pltpu.roll(added, 6, 0), 0.0)
    smoothed_ref[:, half:] = base_ref[:, half:] + jnp.where(edge, pltpu.roll(added, 2, 0), 0.0)


def apply_kernel(bands_total, cells_ref, total_ref, inner_ref, outer_ref, target_ref, band_ref, smoothed_ref, out_ref):
    pooled = total_ref[...] + inner_ref[...] + outer_ref[...]
    pooled = jnp.broadcast_to(pooled, (SUBLANES, LANES))
    counts = pltpu.roll(pooled, LANES - bands_total, 1)
    target = jnp.concatenate([target_ref[...]] * (LANES // bands_total), axis=1)
    table = target - pooled / (counts + 1.0)
    cells = cells_ref[0]
    rows, width = band_ref.shape
    position = iota((rows, LANES), 0) * width + iota((rows, LANES), 1)
    for k in range(width // LANES):
        here = slice(k * LANES, (k + 1) * LANES)
        applied = jnp.take_along_axis(table, band_ref[:, here], axis=1, mode="promise_in_bounds")
        live = position + k * LANES < cells
        out_ref[:, here] = smoothed_ref[:, here] + jnp.where(live, applied, 0.0)


def shards(ensemble, band_index, region_cells, target_means):
    region_count = lax.axis_size("region")
    rank = lax.axis_index("region")
    _, rows, width = ensemble.shape
    bands_total = target_means.shape[1]
    inner_pairs = [(i, i ^ 1) for i in range(region_count)]
    outer_pairs = [(i, ((i + 1) ^ 1) - 1) for i in range(1, region_count - 1)]
    field, band = ensemble[0], band_index[0]
    even = rank % 2 == 0
    first, last = field[:2], field[rows - 2 :]
    outer = lax.ppermute(jnp.where(even, first, last), "region", outer_pairs)
    inner = lax.ppermute(jnp.where(even, last, first), "region", inner_pairs)
    places = jnp.stack([rank == 0, rank == region_count - 1, even]).astype(jnp.int32)
    smem, vmem = pl.BlockSpec(memory_space=pltpu.SMEM), pl.BlockSpec(memory_space=pltpu.VMEM)
    params = pltpu.CompilerParams(vmem_limit_bytes=16 * 2**20)
    tile = jax.ShapeDtypeStruct((rows, width), jnp.float32)
    line = jax.ShapeDtypeStruct((1, 2 * bands_total), jnp.float32)
    cost = pl.CostEstimate(flops=4 * 10**9, bytes_accessed=4 * rows * width * 4, transcendentals=0)
    base, code, prepared = pl.pallas_call(
        functools.partial(prepare_kernel, bands_total),
        out_shape=(tile, jax.ShapeDtypeStruct((rows, width // 2), jnp.int32), line),
        in_specs=[smem, smem, vmem, vmem],
        out_specs=(vmem, vmem, vmem),
        compiler_params=params,
        cost_estimate=cost,
        name="prepare",
    )(region_cells, places, field, band)
    smoothed, stats = pl.pallas_call(
        functools.partial(edges_kernel, bands_total),
        out_shape=(tile, line),
        in_specs=[smem] + [vmem] * 5,
        out_specs=(vmem, vmem),
        compiler_params=params,
        name="edges",
    )(places, inner, outer, base, code, prepared)
    total = lax.all_gather(stats, "member").sum(axis=0)
    outer_total = lax.ppermute(total, "region", outer_pairs)
    inner_total = lax.ppermute(total, "region", inner_pairs)
    out = pl.pallas_call(
        functools.partial(apply_kernel, bands_total),
        out_shape=tile,
        in_specs=[smem] + [vmem] * 6,
        out_specs=vmem,
        compiler_params=params,
        name="apply",
    )(region_cells, total, inner_total, outer_total, target_means, band, smoothed)
    return out[None]


def solution(mesh):
    placed = (
        P("member", "region", None),
        P("member", "region", None),
        P("region"),
        P("region", None),
    )
    return jax.shard_map(
        shards, mesh=mesh, in_specs=placed, out_specs=P("member", "region", None), check_vma=False
    )
```

```python
import functools

import jax
import jax.numpy as jnp
from jax import lax
from jax.experimental import pallas as pl
from jax.experimental.pallas import tpu as pltpu
from jax.sharding import PartitionSpec as P

LANES = 128
SUBLANES = 8
LOW = 16


def iota(shape, axis):
    return lax.broadcasted_iota(jnp.int32, shape, axis)


def rank_flags():
    rank = lax.axis_index("region")
    return rank == 0, rank == lax.axis_size("region") - 1, rank % 2 == 0


def smooth_along(field, kept):
    width = field.shape[1]
    lane = iota(field.shape, 1)

    def shifted(values, by, edge, turn):
        moved = pltpu.roll(values, by, 1)
        return jnp.where(lane == edge, pltpu.roll(moved, turn, 0), moved) if kept else moved

    for _ in range(2):
        field = field + shifted(field, 1, 0, kept)
        field = field + shifted(field, width - 1, width - 1, SUBLANES - kept)
    return field


def bf16_terms(values):
    high = values.astype(jnp.bfloat16).astype(jnp.float32)
    rest = values - high
    middle = rest.astype(jnp.bfloat16).astype(jnp.float32)
    return [high, middle, rest - middle]


def band_blocks(bands_total, code, values, groups):
    blocks = bands_total // LOW
    upper = jnp.floor(code * (1.0 / LOW))
    lower = code - upper * LOW
    terms = bf16_terms(values)
    terms.append(jnp.full(values.shape, 1.0, jnp.float32))
    tiles = [jnp.concatenate(terms[k : k + 2], axis=0).astype(jnp.bfloat16) for k in (0, 2)]
    upper = jnp.concatenate([upper, upper], axis=0).astype(jnp.bfloat16)
    lower = jnp.concatenate([lower, lower - 1.0], axis=0).astype(jnp.bfloat16)
    zero, one = jnp.zeros((), jnp.bfloat16), jnp.ones((), jnp.bfloat16)
    left = jnp.concatenate([jnp.where(upper == a, t, zero) for a in range(blocks) for t in tiles], axis=0)
    right = jnp.concatenate([jnp.where(lower == b, one, zero) for b in range(0, LOW, 2)], axis=0)
    product = lax.dot_general(left, right, (((1,), (1,)), ((), ())), preferred_element_type=jnp.float32)
    sublane, lane = iota((SUBLANES, LANES), 0), iota((SUBLANES, LANES), 1)
    made = []
    for mask, count in groups:
        kept = sublane == lane % SUBLANES
        kept = kept if mask is None else kept & mask
        block = jnp.zeros((SUBLANES, LANES), jnp.float32)
        for a in range(blocks):
            part = [product[(4 * a + k) * SUBLANES : (4 * a + k + 1) * SUBLANES] for k in range(4)]
            sums = jnp.sum(jnp.where(kept, part[0] + (part[1] + part[2]), 0.0), axis=0, keepdims=True)
            block = jnp.where(sublane == 2 * a, sums, block)
            if count:
                counts = jnp.sum(jnp.where(kept, part[3], 0.0), axis=0, keepdims=True)
                block = jnp.where(sublane == 2 * a + 1, counts, block)
        made.append(block)
    return made


def weigh(first, second, even, table):
    slot = iota((SUBLANES, LANES), 0) % len(table[0])
    total = None
    for values, pairs in ((first, table[0]), (second, table[1])):
        weight = jnp.zeros((SUBLANES, LANES), jnp.float32)
        for s, (a, b) in enumerate(pairs):
            weight = jnp.where(slot == s, jnp.where(even, a, b) * (1.0 / 256.0), weight)
        term = values * jnp.concatenate([weight] * (values.shape[1] // LANES), axis=1)
        total = term if total is None else total + term
    return total


def load_kernel(bands_total, field_hbm, band_hbm, target_hbm, inner_ref, field_ref, band_ref, target_ref, target, sems):
    copies = [
        pltpu.make_async_copy(field_hbm, field_ref, sems.at[0]),
        pltpu.make_async_copy(band_hbm, band_ref, sems.at[1]),
        pltpu.make_async_copy(target_hbm, target, sems.at[2]),
    ]
    for copy in copies:
        copy.start()
    _, _, even = rank_flags()
    copies[0].wait()
    rows = field_ref.shape[0]
    inner_ref[...] = jnp.where(even, field_ref[rows - 2 :, :], field_ref[:2, :])
    copies[1].wait()
    copies[2].wait()
    target_ref[:, :bands_total] = target[...]
    target_ref[:, bands_total:] = target[...]


def prepare_kernel(bands_total, cells_ref, center_ref, band_ref, base_ref, code_ref, edge_code_ref, sent_ref, stats_ref):
    at_north, at_south, even = rank_flags()
    center = center_ref[...]
    rows, width = center.shape
    row = iota(center.shape, 0)
    first, last = row == 0, row == rows - 1
    north, south = center[0:1], center[rows - 1 : rows]

    def vertical(field, prior, later):
        up = jnp.where(first, prior, pltpu.roll(field, 1, 0))
        down = jnp.where(last, later, pltpu.roll(field, rows - 1, 0))
        return (up + field) + (field + down)

    once = vertical(center, jnp.where(at_north, north, 0.0), jnp.where(at_south, south, 0.0))
    prior = jnp.where(at_north, once[0:1], north)
    later = jnp.where(at_south, once[rows - 1 : rows], south)
    base = smooth_along(vertical(once, prior, later) * (1.0 / 256.0), 0)
    base_ref[...] = base
    live = row * width + iota(center.shape, 1) < cells_ref[0]
    code = jnp.where(live, band_ref[...], bands_total)
    code_ref[...] = code
    code = code.astype(jnp.float32)
    piece = width // 4
    start = jnp.where(even, 2, 0)
    packed = None
    for q in range(4):
        part = pltpu.roll(code[:, q * piece : (q + 1) * piece], start + 2 * q, 0)
        packed = part if packed is None else jnp.where(iota(part.shape, 0) // 2 == q, part, packed)
    edge_code_ref[...] = packed
    sent_ref[0:2, :] = jnp.where(even, center[:2], center[rows - 2 :])
    sent_ref[2:4, :] = jnp.where(even, code[:2], code[rows - 2 :])
    (stats_ref[...],) = band_blocks(bands_total, code, base, [(None, True)])


def inner_kernel(bands_total, got_ref, code_ref, prepared_ref, edge_ref, added_ref, sent_ref):
    _, _, even = rank_flags()
    piece = got_ref.shape[1] // 4
    quarter = iota((SUBLANES, piece), 0) // 2
    lines = []
    for j in range(2):
        line = jnp.broadcast_to(got_ref[j : j + 1, :piece], (SUBLANES, piece))
        for q in range(1, 4):
            line = jnp.where(quarter == q, got_ref[j : j + 1, q * piece : (q + 1) * piece], line)
        lines.append(line)
    added = weigh(lines[0], lines[1], even, (((1.0, 1.0), (4.0, 0.0)), ((0.0, 4.0), (1.0, 1.0))))
    added = smooth_along(added, 2)
    added_ref[...] = added
    (block,) = band_blocks(bands_total, code_ref[...], added, [(None, False)])
    block = prepared_ref[...] + block
    width = got_ref.shape[1]
    sent_ref[:, :width] = edge_ref[...]
    sent_ref[:, width : width + LANES] = block[:4]
    sent_ref[:, width + LANES :] = block[4:]


def outer_kernel(bands_total, got_ref, sent_ref, base_ref, added_ref, smoothed_ref, blocks_ref):
    at_north, at_south, even = rank_flags()
    rows, width = base_ref.shape
    half = width // 2
    shape = (SUBLANES, half)
    low = iota(shape, 0) < SUBLANES // 2
    slot = iota(shape, 0) % (SUBLANES // 2)

    def row_of(ref, j):
        return jnp.where(low, ref[j : j + 1, :half], ref[j : j + 1, half:width])

    own = slot < 2
    lines = [jnp.where(own, row_of(got_ref, j), row_of(sent_ref, j)) for j in range(2)]
    codes = [row_of(ref, j) for ref in (sent_ref, got_ref) for j in (2, 3)]
    code = jnp.where(own, jnp.where(slot == 0, codes[0], codes[1]), jnp.where(slot == 2, codes[2], codes[3]))
    table = (((1.0, 1.0), (0.0, 4.0), (1.0, 1.0), (4.0, 0.0)), ((4.0, 0.0), (1.0, 1.0), (0.0, 4.0), (1.0, 1.0)))
    added = smooth_along(weigh(lines[0], lines[1], even, table), 4)
    alone = at_north | at_south
    code = jnp.where(alone, float(bands_total), code)
    crossing = iota((SUBLANES, LANES), 0) % 4 >= 2
    own, cross = band_blocks(bands_total, code, added, [(~crossing, False), (crossing, False)])

    def block_of(ref):
        return jnp.concatenate([ref[:, width : width + LANES], ref[:, width + LANES :]], axis=0)

    own = block_of(sent_ref) + own
    cross = block_of(got_ref) + cross
    count = blocks_ref.shape[0]
    for k in range(count):
        blocks_ref[k] = own + jnp.where((k < count // 2) == even, cross, 0.0)
    piece = width // 4
    row = iota((rows, piece), 0)
    inner_start = jnp.where(even, rows - 2, 0)
    outer_start = jnp.where(even, 0, rows - 2)
    inner_row, outer_row = row // 2 == inner_start // 2, row // 2 == outer_start // 2
    for q in range(4):
        here = slice(q * piece, (q + 1) * piece)
        there = slice(q % 2 * piece, (q % 2 + 1) * piece)
        inner = pltpu.roll(added_ref[...], inner_start + (SUBLANES - 2 * q), 0)
        outer = pltpu.roll(added[:, there], outer_start + (SUBLANES - q // 2 * 4), 0)
        smoothed_ref[:, here] = base_ref[:, here] + jnp.where(inner_row, inner, jnp.where(outer_row, outer, 0.0))


def apply_kernel(bands_total, blocks_ref, target_ref, code_ref, smoothed_ref, out_ref):
    pooled = jnp.sum(blocks_ref[...], axis=0)
    for shift in (1, 2, 4):
        pooled = pooled + pltpu.roll(pooled, LANES - shift, 1)
    sublane, lane = iota(pooled.shape, 0), iota(pooled.shape, 1)
    pooled = jnp.take_along_axis(pooled, lane % LOW * SUBLANES, axis=1, mode="promise_in_bounds")
    row = lane % bands_total // LOW * 2
    sums = jnp.sum(jnp.where(sublane == row, pooled, 0.0), axis=0, keepdims=True)
    counts = jnp.sum(jnp.where(sublane == row + 1, pooled, 0.0), axis=0, keepdims=True)
    table = target_ref[...] - sums / (counts + 1.0)
    table = jnp.where(lane < bands_total, table, 0.0)
    for k in range(code_ref.shape[1] // LANES):
        here = slice(k * LANES, (k + 1) * LANES)
        applied = jnp.take_along_axis(table, code_ref[:, here], axis=1, mode="promise_in_bounds")
        out_ref[:, here] = smoothed_ref[:, here] + applied


def shards(ensemble, band_index, region_cells, target_means):
    region_count = lax.axis_size("region")
    _, rows, width = ensemble.shape
    bands_total = target_means.shape[1]
    inner_pairs = [(i, i ^ 1) for i in range(region_count)]
    outer_pairs = [(i, ((i + 1) ^ 1) - 1) for i in range(1, region_count - 1)]
    field, band = ensemble[0], band_index[0]
    vmem = pl.BlockSpec(memory_space=pltpu.VMEM)

    def shape(count, columns, kind=jnp.float32):
        return jax.ShapeDtypeStruct((count, columns), kind)

    tile, block = shape(rows, width), shape(SUBLANES, LANES)

    def call(kernel, name, outs, ins, flops, **more):
        return pl.pallas_call(
            functools.partial(kernel, bands_total),
            out_shape=outs,
            in_specs=ins,
            out_specs=jax.tree.map(lambda _: vmem, outs),
            compiler_params=pltpu.CompilerParams(vmem_limit_bytes=16 * 2**20),
            cost_estimate=pl.CostEstimate(flops=flops, bytes_accessed=2**20, transcendentals=0),
            name=name,
            **more,
        )

    inner_sent, field, band, target = call(
        load_kernel, "load", (shape(2, width), tile, shape(rows, width, jnp.int32), shape(1, 2 * bands_total)),
        [pl.BlockSpec(memory_space=pltpu.HBM)] * 3, 10**6,
        scratch_shapes=[pltpu.VMEM((1, bands_total), jnp.float32), pltpu.SemaphoreType.DMA((3,))],
    )(*[pltpu.with_memory_space_constraint(a, pltpu.HBM) for a in (field, band, target_means)])
    inner_got = lax.ppermute(inner_sent, "region", inner_pairs)
    payload = shape(4, width + 2 * LANES)
    base, code, edge_code, sent, prepared = call(
        prepare_kernel, "prepare",
        (tile, shape(rows, width, jnp.int32), shape(rows, width // 4), shape(4, width), block),
        [pl.BlockSpec(memory_space=pltpu.SMEM), vmem, vmem], 4 * 10**9,
    )(region_cells, field, band)
    added, sent = call(
        inner_kernel, "inner", (shape(rows, width // 4), payload), [vmem] * 4, 10**9
    )(inner_got, edge_code, prepared, sent)
    got = lax.ppermute(sent, "region", outer_pairs)
    members = lax.axis_size("member")
    blocks_out = jax.ShapeDtypeStruct((2 * members, SUBLANES, LANES), jnp.float32)
    smoothed, blocks = call(outer_kernel, "outer", (tile, blocks_out), [vmem] * 4, 10**9)(
        got, sent, base, added
    )
    groups = [[2 * members * k + i for i in range(2 * members)] for k in range(region_count // 2)]
    pieces = lax.all_to_all(blocks, ("region", "member"), 0, 0, axis_index_groups=groups, tiled=True)
    out = call(apply_kernel, "apply", tile, [vmem] * 4, 10**9)(pieces, target, code, smoothed)
    return out[None]


def solution(mesh):
    placed = (
        P("member", "region", None),
        P("member", "region", None),
        P("region"),
        P("region", None),
    )
    return jax.shard_map(
        shards, mesh=mesh, in_specs=placed, out_specs=P("member", "region", None), check_vma=False
    )
```

```python
import functools

import jax
import jax.numpy as jnp
from jax import lax
from jax.experimental import pallas as pl
from jax.experimental.pallas import tpu as pltpu
from jax.sharding import PartitionSpec as P

LANES = 128
SUBLANES = 8
LOW = 16


def iota(shape, axis):
    return lax.broadcasted_iota(jnp.int32, shape, axis)


def rank_flags():
    rank = lax.axis_index("region")
    return rank == 0, rank == lax.axis_size("region") - 1, rank % 2 == 0


def smooth_along(field, kept):
    width = field.shape[1]
    lane = iota(field.shape, 1)

    def shifted(by):
        moved = pltpu.roll(field, by % width, 1)
        if not kept:
            return moved
        crossed = lane < by if by > 0 else lane >= width + by
        return jnp.where(crossed, pltpu.roll(moved, kept if by > 0 else SUBLANES - kept, 0), moved)

    near, far = shifted(1) + shifted(-1), shifted(2) + shifted(-2)
    return far + 4.0 * near + 6.0 * field


def bf16_terms(values):
    high = values.astype(jnp.bfloat16).astype(jnp.float32)
    rest = values - high
    middle = rest.astype(jnp.bfloat16).astype(jnp.float32)
    return [high, middle, rest - middle]


def band_blocks(bands_total, code, values, groups):
    blocks = bands_total // LOW
    upper = jnp.floor(code * (1.0 / LOW))
    lower = code - upper * LOW
    terms = bf16_terms(values)
    terms.append(jnp.full(values.shape, 1.0, jnp.float32))
    tiles = [jnp.concatenate(terms[k : k + 2], axis=0).astype(jnp.bfloat16) for k in (0, 2)]
    upper = jnp.concatenate([upper, upper], axis=0).astype(jnp.bfloat16)
    lower = jnp.concatenate([lower, lower - 1.0], axis=0).astype(jnp.bfloat16)
    zero, one = jnp.zeros((), jnp.bfloat16), jnp.ones((), jnp.bfloat16)
    left = jnp.concatenate([jnp.where(upper == a, t, zero) for a in range(blocks) for t in tiles], axis=0)
    right = jnp.concatenate([jnp.where(lower == b, one, zero) for b in range(0, LOW, 2)], axis=0)
    product = lax.dot_general(left, right, (((1,), (1,)), ((), ())), preferred_element_type=jnp.float32)
    sublane, lane = iota((SUBLANES, LANES), 0), iota((SUBLANES, LANES), 1)
    made = []
    for mask, count in groups:
        kept = sublane == lane % SUBLANES
        kept = kept if mask is None else kept & mask
        block = jnp.zeros((SUBLANES, LANES), jnp.float32)
        for a in range(blocks):
            part = [product[(4 * a + k) * SUBLANES : (4 * a + k + 1) * SUBLANES] for k in range(4)]
            sums = jnp.sum(jnp.where(kept, part[0] + (part[1] + part[2]), 0.0), axis=0, keepdims=True)
            block = jnp.where(sublane == 2 * a, sums, block)
            if count:
                counts = jnp.sum(jnp.where(kept, part[3], 0.0), axis=0, keepdims=True)
                block = jnp.where(sublane == 2 * a + 1, counts, block)
        made.append(block)
    return made


def weigh(first, second, even, table):
    slot = iota((SUBLANES, LANES), 0) % len(table[0])
    total = None
    for values, pairs in ((first, table[0]), (second, table[1])):
        weight = jnp.zeros((SUBLANES, LANES), jnp.float32)
        for s, (a, b) in enumerate(pairs):
            weight = jnp.where(slot == s, jnp.where(even, a, b) * (1.0 / 256.0), weight)
        term = values * jnp.concatenate([weight] * (values.shape[1] // LANES), axis=1)
        total = term if total is None else total + term
    return total


def load_kernel(_, field_hbm, band_hbm, inner_ref, field_ref, band_ref, sems):
    copies = [
        pltpu.make_async_copy(field_hbm, field_ref, sems.at[0]),
        pltpu.make_async_copy(band_hbm, band_ref, sems.at[1]),
    ]
    for copy in copies:
        copy.start()
    _, _, even = rank_flags()
    copies[0].wait()
    rows = field_ref.shape[0]
    inner_ref[...] = jnp.where(even, field_ref[rows - 2 :, :], field_ref[:2, :])
    copies[1].wait()


def prepare_kernel(bands_total, cells_ref, center_ref, band_ref, target_hbm, base_ref, code_ref, edge_code_ref, sent_ref, stats_ref, target_ref, target, sem):
    copy = pltpu.make_async_copy(target_hbm, target, sem)
    copy.start()
    at_north, at_south, even = rank_flags()
    center = center_ref[...]
    rows, width = center.shape
    row = iota(center.shape, 0)
    first, last = row == 0, row == rows - 1
    north, south = center[0:1], center[rows - 1 : rows]

    def vertical(field, prior, later):
        up = jnp.where(first, prior, pltpu.roll(field, 1, 0))
        down = jnp.where(last, later, pltpu.roll(field, rows - 1, 0))
        return (up + field) + (field + down)

    once = vertical(center, jnp.where(at_north, north, 0.0), jnp.where(at_south, south, 0.0))
    prior = jnp.where(at_north, once[0:1], north)
    later = jnp.where(at_south, once[rows - 1 : rows], south)
    base = smooth_along(vertical(once, prior, later) * (1.0 / 256.0), 0)
    base_ref[...] = base
    live = row * width + iota(center.shape, 1) < cells_ref[0]
    code = jnp.where(live, band_ref[...], bands_total)
    code_ref[...] = code
    code = code.astype(jnp.float32)
    piece = width // 4
    start = jnp.where(even, 2, 0)
    packed = None
    for q in range(4):
        part = pltpu.roll(code[:, q * piece : (q + 1) * piece], start + 2 * q, 0)
        packed = part if packed is None else jnp.where(iota(part.shape, 0) // 2 == q, part, packed)
    edge_code_ref[...] = packed
    sent_ref[0:2, :] = jnp.where(even, center[:2], center[rows - 2 :])
    sent_ref[2:4, :] = jnp.where(even, code[:2], code[rows - 2 :])
    (stats_ref[...],) = band_blocks(bands_total, code, base, [(None, True)])
    copy.wait()
    target_ref[:, :bands_total] = target[...]
    target_ref[:, bands_total:] = target[...]


def inner_kernel(bands_total, got_ref, code_ref, prepared_ref, edge_ref, added_ref, sent_ref):
    _, _, even = rank_flags()
    piece = got_ref.shape[1] // 4
    quarter = iota((SUBLANES, piece), 0) // 2
    lines = []
    for j in range(2):
        line = jnp.broadcast_to(got_ref[j : j + 1, :piece], (SUBLANES, piece))
        for q in range(1, 4):
            line = jnp.where(quarter == q, got_ref[j : j + 1, q * piece : (q + 1) * piece], line)
        lines.append(line)
    added = weigh(lines[0], lines[1], even, (((1.0, 1.0), (4.0, 0.0)), ((0.0, 4.0), (1.0, 1.0))))
    added = smooth_along(added, 2)
    added_ref[...] = added
    (block,) = band_blocks(bands_total, code_ref[...], added, [(None, False)])
    block = prepared_ref[...] + block
    width = got_ref.shape[1]
    sent_ref[:, :width] = edge_ref[...]
    sent_ref[:, width : width + LANES] = block[:4]
    sent_ref[:, width + LANES :] = block[4:]


def outer_kernel(bands_total, got_ref, sent_ref, base_ref, added_ref, smoothed_ref, blocks_ref):
    at_north, at_south, even = rank_flags()
    rows, width = base_ref.shape
    half = width // 2
    shape = (SUBLANES, half)
    low = iota(shape, 0) < SUBLANES // 2
    slot = iota(shape, 0) % (SUBLANES // 2)

    def row_of(ref, j):
        return jnp.where(low, ref[j : j + 1, :half], ref[j : j + 1, half:width])

    own = slot < 2
    lines = [jnp.where(own, row_of(got_ref, j), row_of(sent_ref, j)) for j in range(2)]
    codes = [row_of(ref, j) for ref in (sent_ref, got_ref) for j in (2, 3)]
    code = jnp.where(own, jnp.where(slot == 0, codes[0], codes[1]), jnp.where(slot == 2, codes[2], codes[3]))
    table = (((1.0, 1.0), (0.0, 4.0), (1.0, 1.0), (4.0, 0.0)), ((4.0, 0.0), (1.0, 1.0), (0.0, 4.0), (1.0, 1.0)))
    added = smooth_along(weigh(lines[0], lines[1], even, table), 4)
    alone = at_north | at_south
    code = jnp.where(alone, float(bands_total), code)
    crossing = iota((SUBLANES, LANES), 0) % 4 >= 2
    own, cross = band_blocks(bands_total, code, added, [(~crossing, False), (crossing, False)])

    def block_of(ref):
        return jnp.concatenate([ref[:, width : width + LANES], ref[:, width + LANES :]], axis=0)

    own = block_of(sent_ref) + own
    cross = block_of(got_ref) + cross
    count = blocks_ref.shape[0]
    for k in range(count):
        blocks_ref[k] = own + jnp.where((k < count // 2) == even, cross, 0.0)
    piece = width // 4
    row = iota((rows, piece), 0)
    inner_start = jnp.where(even, rows - 2, 0)
    outer_start = jnp.where(even, 0, rows - 2)
    inner_row, outer_row = row // 2 == inner_start // 2, row // 2 == outer_start // 2
    for q in range(4):
        here = slice(q * piece, (q + 1) * piece)
        there = slice(q % 2 * piece, (q % 2 + 1) * piece)
        inner = pltpu.roll(added_ref[...], inner_start + (SUBLANES - 2 * q), 0)
        outer = pltpu.roll(added[:, there], outer_start + (SUBLANES - q // 2 * 4), 0)
        smoothed_ref[:, here] = base_ref[:, here] + jnp.where(inner_row, inner, jnp.where(outer_row, outer, 0.0))


def apply_kernel(bands_total, blocks_ref, target_ref, code_ref, smoothed_ref, out_ref):
    pooled = jnp.sum(blocks_ref[...], axis=0)
    sublane, lane = iota(pooled.shape, 0), iota(pooled.shape, 1)
    parts = [
        jnp.take_along_axis(pooled, lane % LOW * SUBLANES + k, axis=1, mode="promise_in_bounds") for k in range(SUBLANES)
    ]
    while len(parts) > 1:
        parts = [a + b for a, b in zip(parts[::2], parts[1::2])]
    (pooled,) = parts
    row = lane % bands_total // LOW * 2
    sums = jnp.sum(jnp.where(sublane == row, pooled, 0.0), axis=0, keepdims=True)
    counts = jnp.sum(jnp.where(sublane == row + 1, pooled, 0.0), axis=0, keepdims=True)
    table = target_ref[...] - sums / (counts + 1.0)
    table = jnp.where(lane < bands_total, table, 0.0)
    for k in range(code_ref.shape[1] // LANES):
        here = slice(k * LANES, (k + 1) * LANES)
        applied = jnp.take_along_axis(table, code_ref[:, here], axis=1, mode="promise_in_bounds")
        out_ref[:, here] = smoothed_ref[:, here] + applied


def shards(ensemble, band_index, region_cells, target_means):
    region_count = lax.axis_size("region")
    _, rows, width = ensemble.shape
    bands_total = target_means.shape[1]
    inner_pairs = [(i, i ^ 1) for i in range(region_count)]
    outer_pairs = [(i, ((i + 1) ^ 1) - 1) for i in range(1, region_count - 1)]
    field, band = ensemble[0], band_index[0]
    vmem = pl.BlockSpec(memory_space=pltpu.VMEM)

    def shape(count, columns, kind=jnp.float32):
        return jax.ShapeDtypeStruct((count, columns), kind)

    tile, block = shape(rows, width), shape(SUBLANES, LANES)

    def call(kernel, name, outs, ins, flops, **more):
        return pl.pallas_call(
            functools.partial(kernel, bands_total),
            out_shape=outs,
            in_specs=ins,
            out_specs=jax.tree.map(lambda _: vmem, outs),
            compiler_params=pltpu.CompilerParams(vmem_limit_bytes=16 * 2**20),
            cost_estimate=pl.CostEstimate(flops=flops, bytes_accessed=2**20, transcendentals=0),
            name=name,
            **more,
        )

    inner_sent, field, band = call(
        load_kernel, "load", (shape(2, width), tile, shape(rows, width, jnp.int32)),
        [pl.BlockSpec(memory_space=pltpu.HBM)] * 2, 10**6, scratch_shapes=[pltpu.SemaphoreType.DMA((2,))],
    )(*[pltpu.with_memory_space_constraint(a, pltpu.HBM) for a in (field, band)])
    inner_got = lax.ppermute(inner_sent, "region", inner_pairs)
    payload = shape(4, width + 2 * LANES)
    base, code, edge_code, sent, prepared, target = call(
        prepare_kernel, "prepare",
        (tile, shape(rows, width, jnp.int32), shape(rows, width // 4), shape(4, width), block, shape(1, 2 * bands_total)),
        [pl.BlockSpec(memory_space=pltpu.SMEM), vmem, vmem, pl.BlockSpec(memory_space=pltpu.HBM)], 4 * 10**9,
        scratch_shapes=[pltpu.VMEM((1, bands_total), jnp.float32), pltpu.SemaphoreType.DMA],
    )(region_cells, field, band, pltpu.with_memory_space_constraint(target_means, pltpu.HBM))
    added, sent = call(
        inner_kernel, "inner", (shape(rows, width // 4), payload), [vmem] * 4, 10**9
    )(inner_got, edge_code, prepared, sent)
    got = lax.ppermute(sent, "region", outer_pairs)
    members = lax.axis_size("member")
    blocks_out = jax.ShapeDtypeStruct((2 * members, SUBLANES, LANES), jnp.float32)
    smoothed, blocks = call(outer_kernel, "outer", (tile, blocks_out), [vmem] * 4, 10**9)(
        got, sent, base, added
    )
    groups = [[2 * members * k + i for i in range(2 * members)] for k in range(region_count // 2)]
    pieces = lax.all_to_all(blocks, ("region", "member"), 0, 0, axis_index_groups=groups, tiled=True)
    out = call(apply_kernel, "apply", tile, [vmem] * 4, 10**9)(pieces, target, code, smoothed)
    return out[None]


def solution(mesh):
    placed = (
        P("member", "region", None),
        P("member", "region", None),
        P("region"),
        P("region", None),
    )
    return jax.shard_map(
        shards, mesh=mesh, in_specs=placed, out_specs=P("member", "region", None), check_vma=False
    )
```

```python
import functools

import jax
import jax.numpy as jnp
from jax import lax
from jax.experimental import pallas as pl
from jax.experimental.pallas import tpu as pltpu
from jax.sharding import PartitionSpec as P

LANES = 128
SUBLANES = 8
LOW = 16


def iota(shape, axis):
    return lax.broadcasted_iota(jnp.int32, shape, axis)


def rank_flags():
    rank = lax.axis_index("region")
    return rank == 0, rank == lax.axis_size("region") - 1, rank % 2 == 0


def smooth_along(field, kept):
    width = field.shape[1]
    lane = iota((SUBLANES, LANES), 1)

    def shifted(by):
        moved = pltpu.roll(field, by % width, 1)
        if not kept:
            return moved
        edge = moved[:, :LANES] if by > 0 else moved[:, width - LANES :]
        crossed = lane < by if by > 0 else lane >= LANES + by
        edge = jnp.where(crossed, pltpu.roll(edge, kept if by > 0 else SUBLANES - kept, 0), edge)
        pieces = [edge, moved[:, LANES:]] if by > 0 else [moved[:, : width - LANES], edge]
        return jnp.concatenate(pieces, axis=1)

    near, far = shifted(1) + shifted(-1), shifted(2) + shifted(-2)
    return far + 4.0 * near + 6.0 * field


def bf16_terms(values):
    high = values.astype(jnp.bfloat16).astype(jnp.float32)
    rest = values - high
    middle = rest.astype(jnp.bfloat16).astype(jnp.float32)
    return [high, middle, rest - middle]


def band_blocks(bands_total, code, values, groups):
    blocks = bands_total // LOW
    upper = jnp.floor(code * (1.0 / LOW))
    lower = code - upper * LOW
    terms = bf16_terms(values)
    terms.append(jnp.full(values.shape, 1.0, jnp.float32))
    tiles = [jnp.concatenate(terms[k : k + 2], axis=0).astype(jnp.bfloat16) for k in (0, 2)]
    upper = jnp.concatenate([upper, upper], axis=0).astype(jnp.bfloat16)
    lower = jnp.concatenate([lower, lower - 1.0], axis=0).astype(jnp.bfloat16)
    zero, one = jnp.zeros((), jnp.bfloat16), jnp.ones((), jnp.bfloat16)
    left = jnp.concatenate([jnp.where(upper == a, t, zero) for a in range(blocks) for t in tiles], axis=0)
    right = jnp.concatenate([jnp.where(lower == b, one, zero) for b in range(0, LOW, 2)], axis=0)
    product = lax.dot_general(left, right, (((1,), (1,)), ((), ())), preferred_element_type=jnp.float32)
    sublane, lane = iota((SUBLANES, LANES), 0), iota((SUBLANES, LANES), 1)
    made = []
    for mask, count in groups:
        kept = sublane == lane % SUBLANES
        kept = kept if mask is None else kept & mask
        block = jnp.zeros((SUBLANES, LANES), jnp.float32)
        for a in range(blocks):
            part = [product[(4 * a + k) * SUBLANES : (4 * a + k + 1) * SUBLANES] for k in range(4)]
            sums = jnp.sum(jnp.where(kept, part[0] + (part[1] + part[2]), 0.0), axis=0, keepdims=True)
            block = jnp.where(sublane == 2 * a, sums, block)
            if count:
                counts = jnp.sum(jnp.where(kept, part[3], 0.0), axis=0, keepdims=True)
                block = jnp.where(sublane == 2 * a + 1, counts, block)
        made.append(block)
    return made


def weigh(first, second, even, table):
    slot = iota((SUBLANES, LANES), 0) % len(table[0])
    total = None
    for values, pairs in ((first, table[0]), (second, table[1])):
        weight = jnp.zeros((SUBLANES, LANES), jnp.float32)
        for s, (a, b) in enumerate(pairs):
            weight = jnp.where(slot == s, jnp.where(even, a, b) * (1.0 / 256.0), weight)
        term = values * jnp.concatenate([weight] * (values.shape[1] // LANES), axis=1)
        total = term if total is None else total + term
    return total


def load_kernel(_, field_hbm, band_hbm, inner_ref, field_ref, band_ref, sems):
    copies = [
        pltpu.make_async_copy(field_hbm, field_ref, sems.at[0]),
        pltpu.make_async_copy(band_hbm, band_ref, sems.at[1]),
    ]
    for copy in copies:
        copy.start()
    _, _, even = rank_flags()
    copies[0].wait()
    rows = field_ref.shape[0]
    inner_ref[...] = jnp.where(even, field_ref[rows - 2 :, :], field_ref[:2, :])
    copies[1].wait()


def prepare_kernel(bands_total, cells_ref, center_ref, band_ref, target_hbm, base_ref, code_ref, edge_code_ref, sent_ref, stats_ref, target_ref, target, sem):
    copy = pltpu.make_async_copy(target_hbm, target, sem)
    copy.start()
    at_north, at_south, even = rank_flags()
    center = center_ref[...]
    rows, width = center.shape
    row = iota(center.shape, 0)
    first, last = row == 0, row == rows - 1
    north, south = center[0:1], center[rows - 1 : rows]

    def vertical(field, prior, later):
        up = jnp.where(first, prior, pltpu.roll(field, 1, 0))
        down = jnp.where(last, later, pltpu.roll(field, rows - 1, 0))
        return (up + field) + (field + down)

    once = vertical(center, jnp.where(at_north, north, 0.0), jnp.where(at_south, south, 0.0))
    prior = jnp.where(at_north, once[0:1], north)
    later = jnp.where(at_south, once[rows - 1 : rows], south)
    base = smooth_along(vertical(once, prior, later) * (1.0 / 256.0), 0)
    base_ref[...] = base
    live = row * width + iota(center.shape, 1) < cells_ref[0]
    code = jnp.where(live, band_ref[...], bands_total)
    code_ref[...] = code
    code = code.astype(jnp.float32)
    piece = width // 4
    start = jnp.where(even, 2, 0)
    packed = None
    for q in range(4):
        part = pltpu.roll(code[:, q * piece : (q + 1) * piece], start + 2 * q, 0)
        packed = part if packed is None else jnp.where(iota(part.shape, 0) // 2 == q, part, packed)
    edge_code_ref[...] = packed
    sent_ref[0:2, :] = jnp.where(even, center[:2], center[rows - 2 :])
    sent_ref[2:4, :] = jnp.where(even, code[:2], code[rows - 2 :])
    (stats_ref[...],) = band_blocks(bands_total, code, base, [(None, True)])
    copy.wait()
    target_ref[:, :bands_total] = target[...]
    target_ref[:, bands_total:] = target[...]


def inner_kernel(bands_total, got_ref, code_ref, prepared_ref, edge_ref, added_ref, sent_ref):
    _, _, even = rank_flags()
    piece = got_ref.shape[1] // 4
    quarter = iota((SUBLANES, piece), 0) // 2
    lines = []
    for j in range(2):
        line = jnp.broadcast_to(got_ref[j : j + 1, :piece], (SUBLANES, piece))
        for q in range(1, 4):
            line = jnp.where(quarter == q, got_ref[j : j + 1, q * piece : (q + 1) * piece], line)
        lines.append(line)
    added = weigh(lines[0], lines[1], even, (((1.0, 1.0), (4.0, 0.0)), ((0.0, 4.0), (1.0, 1.0))))
    added = smooth_along(added, 2)
    added_ref[...] = added
    (block,) = band_blocks(bands_total, code_ref[...], added, [(None, False)])
    block = prepared_ref[...] + block
    width = got_ref.shape[1]
    sent_ref[:, :width] = edge_ref[...]
    sent_ref[:, width : width + LANES] = block[:4]
    sent_ref[:, width + LANES :] = block[4:]


def outer_kernel(bands_total, got_ref, sent_ref, outer_added_ref, blocks_ref):
    at_north, at_south, even = rank_flags()
    width = got_ref.shape[1] - 2 * LANES
    half = width // 2
    shape = (SUBLANES, half)
    low = iota(shape, 0) < SUBLANES // 2
    slot = iota(shape, 0) % (SUBLANES // 2)

    def row_of(ref, j):
        return jnp.where(low, ref[j : j + 1, :half], ref[j : j + 1, half:width])

    own = slot < 2
    lines = [jnp.where(own, row_of(got_ref, j), row_of(sent_ref, j)) for j in range(2)]
    codes = [row_of(ref, j) for ref in (sent_ref, got_ref) for j in (2, 3)]
    code = jnp.where(own, jnp.where(slot == 0, codes[0], codes[1]), jnp.where(slot == 2, codes[2], codes[3]))
    table = (((1.0, 1.0), (0.0, 4.0), (1.0, 1.0), (4.0, 0.0)), ((4.0, 0.0), (1.0, 1.0), (0.0, 4.0), (1.0, 1.0)))
    added = smooth_along(weigh(lines[0], lines[1], even, table), 4)
    alone = at_north | at_south
    code = jnp.where(alone, float(bands_total), code)
    crossing = iota((SUBLANES, LANES), 0) % 4 >= 2
    own, cross = band_blocks(bands_total, code, added, [(~crossing, False), (crossing, False)])

    def block_of(ref):
        return jnp.concatenate([ref[:, width : width + LANES], ref[:, width + LANES :]], axis=0)

    own = block_of(sent_ref) + own
    cross = block_of(got_ref) + cross
    count = blocks_ref.shape[0]
    for k in range(count):
        blocks_ref[k] = own + jnp.where((k < count // 2) == even, cross, 0.0)
    outer_added_ref[...] = added


def apply_kernel(bands_total, blocks_ref, target_ref, code_ref, base_ref, added_ref, outer_ref, out_hbm, out, sems):
    pooled = jnp.sum(blocks_ref[...], axis=0)
    sublane, lane = iota(pooled.shape, 0), iota(pooled.shape, 1)
    parts = [
        jnp.take_along_axis(pooled, lane % LOW * SUBLANES + k, axis=1, mode="promise_in_bounds") for k in range(SUBLANES)
    ]
    while len(parts) > 1:
        parts = [a + b for a, b in zip(parts[::2], parts[1::2])]
    (pooled,) = parts
    row = lane % bands_total // LOW * 2
    sums = jnp.sum(jnp.where(sublane == row, pooled, 0.0), axis=0, keepdims=True)
    counts = jnp.sum(jnp.where(sublane == row + 1, pooled, 0.0), axis=0, keepdims=True)
    table = target_ref[...] - sums / (counts + 1.0)
    table = jnp.where(lane < bands_total, table, 0.0)
    _, _, even = rank_flags()
    rows, width = base_ref.shape
    inner_start = jnp.where(even, rows - 2, 0)
    outer_start = jnp.where(even, 0, rows - 2)
    inner_row, outer_row = sublane // 2 == inner_start // 2, sublane // 2 == outer_start // 2
    piece = width // 4
    copies = []
    for q in range(4):
        for k in range(piece // LANES):
            there = slice(k * LANES, (k + 1) * LANES)
            far = slice(q % 2 * piece + k * LANES, q % 2 * piece + (k + 1) * LANES)
            here = slice(q * piece + k * LANES, q * piece + (k + 1) * LANES)
            inner = pltpu.roll(added_ref[:, there], inner_start + (SUBLANES - 2 * q), 0)
            outer = pltpu.roll(outer_ref[:, far], outer_start + (SUBLANES - q // 2 * 4), 0)
            smoothed = base_ref[:, here] + jnp.where(inner_row, inner, jnp.where(outer_row, outer, 0.0))
            applied = jnp.take_along_axis(table, code_ref[:, here], axis=1, mode="promise_in_bounds")
            out[:, here] = smoothed + applied
        whole = slice(q * piece, (q + 1) * piece)
        copies.append(pltpu.make_async_copy(out.at[:, whole], out_hbm.at[:, whole], sems.at[q]))
        copies[-1].start()
    for copy in copies:
        copy.wait()


def shards(ensemble, band_index, region_cells, target_means):
    region_count = lax.axis_size("region")
    _, rows, width = ensemble.shape
    bands_total = target_means.shape[1]
    inner_pairs = [(i, i ^ 1) for i in range(region_count)]
    outer_pairs = [(i, ((i + 1) ^ 1) - 1) for i in range(1, region_count - 1)]
    field, band = ensemble[0], band_index[0]
    vmem = pl.BlockSpec(memory_space=pltpu.VMEM)

    def shape(count, columns, kind=jnp.float32):
        return jax.ShapeDtypeStruct((count, columns), kind)

    tile, block = shape(rows, width), shape(SUBLANES, LANES)

    def call(kernel, name, outs, ins, flops, out_space=vmem, **more):
        return pl.pallas_call(
            functools.partial(kernel, bands_total),
            out_shape=outs,
            in_specs=ins,
            out_specs=jax.tree.map(lambda _: out_space, outs),
            compiler_params=pltpu.CompilerParams(vmem_limit_bytes=16 * 2**20),
            cost_estimate=pl.CostEstimate(flops=flops, bytes_accessed=2**20, transcendentals=0),
            name=name,
            **more,
        )

    inner_sent, field, band = call(
        load_kernel, "load", (shape(2, width), tile, shape(rows, width, jnp.int32)),
        [pl.BlockSpec(memory_space=pltpu.HBM)] * 2, 10**6, scratch_shapes=[pltpu.SemaphoreType.DMA((2,))],
    )(*[pltpu.with_memory_space_constraint(a, pltpu.HBM) for a in (field, band)])
    inner_got = lax.ppermute(inner_sent, "region", inner_pairs)
    payload = shape(4, width + 2 * LANES)
    base, code, edge_code, sent, prepared, target = call(
        prepare_kernel, "prepare",
        (tile, shape(rows, width, jnp.int32), shape(rows, width // 4), shape(4, width), block, shape(1, 2 * bands_total)),
        [pl.BlockSpec(memory_space=pltpu.SMEM), vmem, vmem, pl.BlockSpec(memory_space=pltpu.HBM)], 4 * 10**9,
        scratch_shapes=[pltpu.VMEM((1, bands_total), jnp.float32), pltpu.SemaphoreType.DMA],
    )(region_cells, field, band, pltpu.with_memory_space_constraint(target_means, pltpu.HBM))
    added, sent = call(
        inner_kernel, "inner", (shape(rows, width // 4), payload), [vmem] * 4, 10**9
    )(inner_got, edge_code, prepared, sent)
    got = lax.ppermute(sent, "region", outer_pairs)
    members = lax.axis_size("member")
    blocks_out = jax.ShapeDtypeStruct((2 * members, SUBLANES, LANES), jnp.float32)
    outer_added, blocks = call(outer_kernel, "outer", (shape(rows, width // 2), blocks_out), [vmem] * 2, 10**9)(
        got, sent
    )
    groups = [[2 * members * k + i for i in range(2 * members)] for k in range(region_count // 2)]
    pieces = lax.all_to_all(blocks, ("region", "member"), 0, 0, axis_index_groups=groups, tiled=True)
    out = call(
        apply_kernel, "apply", tile, [vmem] * 6, 10**9, pl.BlockSpec(memory_space=pltpu.HBM),
        scratch_shapes=[pltpu.VMEM((rows, width), jnp.float32), pltpu.SemaphoreType.DMA((4,))],
    )(
        pieces, target, code, base, added, outer_added
    )
    return out[None]


def solution(mesh):
    placed = (
        P("member", "region", None),
        P("member", "region", None),
        P("region"),
        P("region", None),
    )
    return jax.shard_map(
        shards, mesh=mesh, in_specs=placed, out_specs=P("member", "region", None), check_vma=False
    )
```

```python
import functools

import jax
import jax.numpy as jnp
from jax import lax
from jax.experimental import pallas as pl
from jax.experimental.pallas import tpu as pltpu
from jax.sharding import PartitionSpec as P

LANES = 128
SUBLANES = 8
LOW = 16


def iota(shape, axis):
    return lax.broadcasted_iota(jnp.int32, shape, axis)


def rank_flags():
    rank = lax.axis_index("region")
    return rank == 0, rank == lax.axis_size("region") - 1, rank % 2 == 0


def smooth_along(field, kept):
    width = field.shape[1]
    lane = iota((SUBLANES, LANES), 1)

    def shifted(by):
        moved = pltpu.roll(field, by % width, 1)
        if not kept:
            return moved
        edge = moved[:, :LANES] if by > 0 else moved[:, width - LANES :]
        crossed = lane < by if by > 0 else lane >= LANES + by
        edge = jnp.where(crossed, pltpu.roll(edge, kept if by > 0 else SUBLANES - kept, 0), edge)
        pieces = [edge, moved[:, LANES:]] if by > 0 else [moved[:, : width - LANES], edge]
        return jnp.concatenate(pieces, axis=1)

    near, far = shifted(1) + shifted(-1), shifted(2) + shifted(-2)
    return far + 4.0 * near + 6.0 * field


def bf16_terms(values):
    high = values.astype(jnp.bfloat16).astype(jnp.float32)
    rest = values - high
    middle = rest.astype(jnp.bfloat16).astype(jnp.float32)
    return [high, middle, rest - middle]


def low_columns(code):
    lower = code - jnp.floor(code * (1.0 / LOW)) * LOW
    lower = jnp.concatenate([lower, lower - 1.0], axis=0).astype(jnp.bfloat16)
    zero, one = jnp.zeros((), jnp.bfloat16), jnp.ones((), jnp.bfloat16)
    return jnp.concatenate([jnp.where(lower == b, one, zero) for b in range(0, LOW, 2)], axis=0)


def band_blocks(bands_total, code, values, groups, right=None):
    blocks = bands_total // LOW
    upper = jnp.floor(code * (1.0 / LOW))
    terms = bf16_terms(values)
    terms.append(jnp.full(values.shape, 1.0, jnp.float32))
    tiles = [jnp.concatenate(terms[k : k + 2], axis=0).astype(jnp.bfloat16) for k in (0, 2)]
    upper = jnp.concatenate([upper, upper], axis=0).astype(jnp.bfloat16)
    zero = jnp.zeros((), jnp.bfloat16)
    left = jnp.concatenate([jnp.where(upper == a, t, zero) for a in range(blocks) for t in tiles], axis=0)
    right = low_columns(code) if right is None else right
    product = lax.dot_general(left, right, (((1,), (1,)), ((), ())), preferred_element_type=jnp.float32)
    sublane, lane = iota((SUBLANES, LANES), 0), iota((SUBLANES, LANES), 1)
    made = []
    for mask, count in groups:
        kept = sublane == lane % SUBLANES
        kept = kept if mask is None else kept & mask
        block = jnp.zeros((SUBLANES, LANES), jnp.float32)
        for a in range(blocks):
            part = [product[(4 * a + k) * SUBLANES : (4 * a + k + 1) * SUBLANES] for k in range(4)]
            sums = jnp.sum(jnp.where(kept, part[0] + (part[1] + part[2]), 0.0), axis=0, keepdims=True)
            block = jnp.where(sublane == 2 * a, sums, block)
            if count:
                counts = jnp.sum(jnp.where(kept, part[3], 0.0), axis=0, keepdims=True)
                block = jnp.where(sublane == 2 * a + 1, counts, block)
        made.append(block)
    return made


def weigh(first, second, even, table):
    slot = iota((SUBLANES, LANES), 0) % len(table[0])
    total = None
    for values, pairs in ((first, table[0]), (second, table[1])):
        weight = jnp.zeros((SUBLANES, LANES), jnp.float32)
        for s, (a, b) in enumerate(pairs):
            weight = jnp.where(slot == s, jnp.where(even, a, b) * (1.0 / 256.0), weight)
        term = values * jnp.concatenate([weight] * (values.shape[1] // LANES), axis=1)
        total = term if total is None else total + term
    return total


def load_kernel(_, field_hbm, band_hbm, inner_ref, field_ref, band_ref, sems):
    copies = [
        pltpu.make_async_copy(field_hbm, field_ref, sems.at[0]),
        pltpu.make_async_copy(band_hbm, band_ref, sems.at[1]),
    ]
    for copy in copies:
        copy.start()
    _, _, even = rank_flags()
    copies[0].wait()
    rows = field_ref.shape[0]
    inner_ref[...] = jnp.where(even, field_ref[rows - 2 :, :], field_ref[:2, :])
    copies[1].wait()


def prepare_kernel(bands_total, cells_ref, center_ref, band_ref, target_hbm, base_ref, code_ref, edge_code_ref, sent_ref, stats_ref, target_ref, columns_ref, target, sem):
    copy = pltpu.make_async_copy(target_hbm, target, sem)
    copy.start()
    at_north, at_south, even = rank_flags()
    center = center_ref[...]
    rows, width = center.shape
    row = iota(center.shape, 0)
    first, last = row == 0, row == rows - 1
    north, south = center[0:1], center[rows - 1 : rows]

    def vertical(field, prior, later):
        up = jnp.where(first, prior, pltpu.roll(field, 1, 0))
        down = jnp.where(last, later, pltpu.roll(field, rows - 1, 0))
        return (up + field) + (field + down)

    once = vertical(center, jnp.where(at_north, north, 0.0), jnp.where(at_south, south, 0.0))
    prior = jnp.where(at_north, once[0:1], north)
    later = jnp.where(at_south, once[rows - 1 : rows], south)
    base = smooth_along(vertical(once, prior, later) * (1.0 / 256.0), 0)
    base_ref[...] = base
    live = row * width + iota(center.shape, 1) < cells_ref[0]
    code = jnp.where(live, band_ref[...], bands_total)
    code_ref[...] = code
    code = code.astype(jnp.float32)
    piece = width // 4
    start = jnp.where(even, 2, 0)
    packed = None
    for q in range(4):
        part = pltpu.roll(code[:, q * piece : (q + 1) * piece], start + 2 * q, 0)
        packed = part if packed is None else jnp.where(iota(part.shape, 0) // 2 == q, part, packed)
    edge_code_ref[...] = packed
    columns_ref[...] = low_columns(packed)
    sent_ref[0:2, :] = jnp.where(even, center[:2], center[rows - 2 :])
    sent_ref[2:4, :] = jnp.where(even, code[:2], code[rows - 2 :])
    (stats_ref[...],) = band_blocks(bands_total, code, base, [(None, True)])
    copy.wait()
    target_ref[:, :bands_total] = target[...]
    target_ref[:, bands_total:] = target[...]


def inner_kernel(bands_total, got_ref, code_ref, prepared_ref, edge_ref, columns_ref, added_ref, sent_ref):
    _, _, even = rank_flags()
    piece = got_ref.shape[1] // 4
    quarter = iota((SUBLANES, piece), 0) // 2
    lines = []
    for j in range(2):
        line = jnp.broadcast_to(got_ref[j : j + 1, :piece], (SUBLANES, piece))
        for q in range(1, 4):
            line = jnp.where(quarter == q, got_ref[j : j + 1, q * piece : (q + 1) * piece], line)
        lines.append(line)
    added = weigh(lines[0], lines[1], even, (((1.0, 1.0), (4.0, 0.0)), ((0.0, 4.0), (1.0, 1.0))))
    added = smooth_along(added, 2)
    added_ref[...] = added
    (block,) = band_blocks(bands_total, code_ref[...], added, [(None, False)], columns_ref[...])
    block = prepared_ref[...] + block
    width = got_ref.shape[1]
    sent_ref[:, :width] = edge_ref[...]
    sent_ref[:, width : width + LANES] = block[:4]
    sent_ref[:, width + LANES :] = block[4:]


def outer_kernel(bands_total, got_ref, sent_ref, outer_added_ref, blocks_ref):
    at_north, at_south, even = rank_flags()
    width = got_ref.shape[1] - 2 * LANES
    half = width // 2
    shape = (SUBLANES, half)
    low = iota(shape, 0) < SUBLANES // 2
    slot = iota(shape, 0) % (SUBLANES // 2)

    def row_of(ref, j):
        return jnp.where(low, ref[j : j + 1, :half], ref[j : j + 1, half:width])

    own = slot < 2
    lines = [jnp.where(own, row_of(got_ref, j), row_of(sent_ref, j)) for j in range(2)]
    codes = [row_of(ref, j) for ref in (sent_ref, got_ref) for j in (2, 3)]
    code = jnp.where(own, jnp.where(slot == 0, codes[0], codes[1]), jnp.where(slot == 2, codes[2], codes[3]))
    table = (((1.0, 1.0), (0.0, 4.0), (1.0, 1.0), (4.0, 0.0)), ((4.0, 0.0), (1.0, 1.0), (0.0, 4.0), (1.0, 1.0)))
    added = smooth_along(weigh(lines[0], lines[1], even, table), 4)
    alone = at_north | at_south
    code = jnp.where(alone, float(bands_total), code)
    crossing = iota((SUBLANES, LANES), 0) % 4 >= 2
    own, cross = band_blocks(bands_total, code, added, [(~crossing, False), (crossing, False)])

    def block_of(ref):
        return jnp.concatenate([ref[:, width : width + LANES], ref[:, width + LANES :]], axis=0)

    own = block_of(sent_ref) + own
    cross = block_of(got_ref) + cross
    count = blocks_ref.shape[0]
    for k in range(count):
        blocks_ref[k] = own + jnp.where((k < count // 2) == even, cross, 0.0)
    outer_added_ref[...] = added


def apply_kernel(bands_total, blocks_ref, target_ref, code_ref, base_ref, added_ref, outer_ref, out_hbm, out, sems):
    pooled = jnp.sum(blocks_ref[...], axis=0)
    sublane, lane = iota(pooled.shape, 0), iota(pooled.shape, 1)
    parts = [
        jnp.take_along_axis(pooled, lane % LOW * SUBLANES + k, axis=1, mode="promise_in_bounds") for k in range(SUBLANES)
    ]
    while len(parts) > 1:
        parts = [a + b for a, b in zip(parts[::2], parts[1::2])]
    (pooled,) = parts
    row = lane % bands_total // LOW * 2
    sums = jnp.sum(jnp.where(sublane == row, pooled, 0.0), axis=0, keepdims=True)
    counts = jnp.sum(jnp.where(sublane == row + 1, pooled, 0.0), axis=0, keepdims=True)
    table = target_ref[...] - sums / (counts + 1.0)
    table = jnp.where(lane < bands_total, table, 0.0)
    _, _, even = rank_flags()
    rows, width = base_ref.shape
    inner_start = jnp.where(even, rows - 2, 0)
    outer_start = jnp.where(even, 0, rows - 2)
    inner_row, outer_row = sublane // 2 == inner_start // 2, sublane // 2 == outer_start // 2
    piece = width // 4
    copies = []
    for q in range(4):
        for k in range(piece // LANES):
            there = slice(k * LANES, (k + 1) * LANES)
            far = slice(q % 2 * piece + k * LANES, q % 2 * piece + (k + 1) * LANES)
            here = slice(q * piece + k * LANES, q * piece + (k + 1) * LANES)
            inner = pltpu.roll(added_ref[:, there], inner_start + (SUBLANES - 2 * q), 0)
            outer = pltpu.roll(outer_ref[:, far], outer_start + (SUBLANES - q // 2 * 4), 0)
            smoothed = base_ref[:, here] + jnp.where(inner_row, inner, jnp.where(outer_row, outer, 0.0))
            applied = jnp.take_along_axis(table, code_ref[:, here], axis=1, mode="promise_in_bounds")
            out[:, here] = smoothed + applied
        whole = slice(q * piece, (q + 1) * piece)
        copies.append(pltpu.make_async_copy(out.at[:, whole], out_hbm.at[:, whole], sems.at[q]))
        copies[-1].start()
    for copy in copies:
        copy.wait()


def shards(ensemble, band_index, region_cells, target_means):
    region_count = lax.axis_size("region")
    _, rows, width = ensemble.shape
    bands_total = target_means.shape[1]
    inner_pairs = [(i, i ^ 1) for i in range(region_count)]
    outer_pairs = [(i, ((i + 1) ^ 1) - 1) for i in range(1, region_count - 1)]
    field, band = ensemble[0], band_index[0]
    vmem = pl.BlockSpec(memory_space=pltpu.VMEM)

    def shape(count, columns, kind=jnp.float32):
        return jax.ShapeDtypeStruct((count, columns), kind)

    tile, block = shape(rows, width), shape(SUBLANES, LANES)

    def call(kernel, name, outs, ins, flops, out_space=vmem, **more):
        return pl.pallas_call(
            functools.partial(kernel, bands_total),
            out_shape=outs,
            in_specs=ins,
            out_specs=jax.tree.map(lambda _: out_space, outs),
            compiler_params=pltpu.CompilerParams(vmem_limit_bytes=16 * 2**20),
            cost_estimate=pl.CostEstimate(flops=flops, bytes_accessed=2**20, transcendentals=0),
            name=name,
            **more,
        )

    inner_sent, field, band = call(
        load_kernel, "load", (shape(2, width), tile, shape(rows, width, jnp.int32)),
        [pl.BlockSpec(memory_space=pltpu.HBM)] * 2, 10**6, scratch_shapes=[pltpu.SemaphoreType.DMA((2,))],
    )(*[pltpu.with_memory_space_constraint(a, pltpu.HBM) for a in (field, band)])
    inner_got = lax.ppermute(inner_sent, "region", inner_pairs)
    payload = shape(4, width + 2 * LANES)
    base, code, edge_code, sent, prepared, target, columns = call(
        prepare_kernel, "prepare",
        (tile, shape(rows, width, jnp.int32), shape(rows, width // 4), shape(4, width), block, shape(1, 2 * bands_total),
         shape(LOW * SUBLANES, width // 4, jnp.bfloat16)),
        [pl.BlockSpec(memory_space=pltpu.SMEM), vmem, vmem, pl.BlockSpec(memory_space=pltpu.HBM)], 4 * 10**9,
        scratch_shapes=[pltpu.VMEM((1, bands_total), jnp.float32), pltpu.SemaphoreType.DMA],
    )(region_cells, field, band, pltpu.with_memory_space_constraint(target_means, pltpu.HBM))
    added, sent = call(
        inner_kernel, "inner", (shape(rows, width // 4), payload), [vmem] * 5, 10**9
    )(inner_got, edge_code, prepared, sent, columns)
    got = lax.ppermute(sent, "region", outer_pairs)
    members = lax.axis_size("member")
    blocks_out = jax.ShapeDtypeStruct((2 * members, SUBLANES, LANES), jnp.float32)
    outer_added, blocks = call(outer_kernel, "outer", (shape(rows, width // 2), blocks_out), [vmem] * 2, 10**9)(
        got, sent
    )
    groups = [[2 * members * k + i for i in range(2 * members)] for k in range(region_count // 2)]
    pieces = lax.all_to_all(blocks, ("region", "member"), 0, 0, axis_index_groups=groups, tiled=True)
    out = call(
        apply_kernel, "apply", tile, [vmem] * 6, 10**9, pl.BlockSpec(memory_space=pltpu.HBM),
        scratch_shapes=[pltpu.VMEM((rows, width), jnp.float32), pltpu.SemaphoreType.DMA((4,))],
    )(
        pieces, target, code, base, added, outer_added
    )
    return out[None]


def solution(mesh):
    placed = (
        P("member", "region", None),
        P("member", "region", None),
        P("region"),
        P("region", None),
    )
    return jax.shard_map(
        shards, mesh=mesh, in_specs=placed, out_specs=P("member", "region", None), check_vma=False
    )
```
